128 devices in a mesh: seq: 32 (over x, z, core), section: 4 (over y).
Axes of the slice: x: 4, y: 4, z: 4, core: 2. Of those that a mesh axis runs over, the one named last changes fastest.
Arguments:
- grad_top: bfloat16 [4, 16384, 2560], P('section', 'seq'), may hold values from -6 to 6
- in_weight: bfloat16 [2560, 2560], P(('seq', 'section')), may hold values from -0.125 to 0.125
- out_weight: bfloat16 [2560, 2560], P(('seq', 'section')), may hold values from -0.125 to 0.125
- gate_branch: bfloat16 [4, 16384, 2560], P('section', 'seq'), may hold values from -6 to 6
- write_vec: bfloat16 [4, 16384, 128], P('section', 'seq'), may hold values from -0.59765625 to 0.59765625
- read_vec: bfloat16 [4, 16384, 128], P('section', 'seq'), may hold values from -6 to 6
- log_decay: float32 [4, 40, 16384], P('section', None, 'seq'), may hold values from -1 to 0
- step_size: float32 [4, 40, 16384], P('section', None, 'seq'), may hold values from 0.005 to 0.05
- skip_gain: float32 [40], replicated, may hold values from 0.5 to 1.5
- visual_pos: int32 [4, 32, 64], P('section', 'seq'), may hold values from 0 to 511, as said below
- visual_count: int32 [4, 32], P('section'), may hold values from 2 to 64, as said below
- visual_owner: int32 [4, 32, 64], P('section'), may hold values from 0 to 31, as said below
- visual_patch: int32 [4, 32, 64], P('section'), may hold values from 0 to 63, as said below
Outputs:
- layer_grads: bfloat16 [4, 16384, 2560], P('section', 'seq')
- patch_grads: bfloat16 [4, 2048, 2560], P('section', 'seq')
The draws below stay inside these ranges and needn't reach their ends.
Inputs may be any that keep to these rules, and one draw needn't show every extreme that they name: `visual_pos`: the 64 positions of one shard are distinct; only the first visual_count of them hold visual tokens. `visual_count`: in every sequence some shard has all 64 slots live. `visual_owner`: of the slots of one shard at most 2 name one owner; in every sequence one owner is named by 2 live slots of every shard. `visual_patch`: slots of one sequence that name the same owner name distinct patches.
All inputs are finite; a program needn't handle non-finite values.
Results may differ from the reference program's by a relative error of at most 0.014.
Values may be sent and summed in bfloat16 or wider, within the bound.
No kernel may reach another device: no remote copies, remote signals or barrier semaphores. Data moves between devices by JAX's collectives and lax.ppermute only.
A program may use at most 192 MiB of HBM per device.

```python
import math
import jax
import jax.numpy as jnp
from jax import lax

D = 2560
LOCAL_HEADS = 40
P_SIZE = 64
N = 128
GROUP = 256
TOK_DEV = 512
CAP = 2
SECTION_SEQS = 4
HP = 2560
SEQUENCE_TOKENS = 16384
VSLOT = 64
PATCH_OWN = 64
N_SEQ = 32


def draw_log_decay(key, part):
    random_keys = jax.random.split(jax.random.fold_in(key, 3), 6)
    shape = (SECTION_SEQS, LOCAL_HEADS, SEQUENCE_TOKENS)
    fast_share = 0.5
    fast_head = jax.random.uniform(random_keys[0], (SECTION_SEQS, LOCAL_HEADS, 1)) < fast_share
    slow_rate = jnp.exp(jax.random.uniform(random_keys[1], (SECTION_SEQS, LOCAL_HEADS, 1), minval=jnp.log(0.2), maxval=jnp.log(0.7))) / SEQUENCE_TOKENS
    fast_rate = jnp.exp(jax.random.uniform(random_keys[2], (SECTION_SEQS, LOCAL_HEADS, 1), minval=jnp.log(1.0 / 50.0), maxval=jnp.log(1.0 / 30.0)))
    head_decay_rate = jnp.where(fast_head, fast_rate, slow_rate)
    multiplier = jax.random.uniform(random_keys[3], shape, minval=0.5, maxval=2.0)
    spike_position = jax.random.randint(random_keys[4], (SECTION_SEQS, LOCAL_HEADS, 2), 0, SEQUENCE_TOKENS)
    spike_penalty = jnp.log(jax.random.uniform(random_keys[5], (SECTION_SEQS, LOCAL_HEADS, 2), minval=0.5, maxval=0.8))
    token_locations = jnp.arange(SEQUENCE_TOKENS)
    spike_events = jnp.where(token_locations == spike_position[..., 0:1], spike_penalty[..., 0:1], 0.0)
    spike_events = spike_events + jnp.where(token_locations == spike_position[..., 1:2], spike_penalty[..., 1:2], 0.0)
    return (-head_decay_rate * multiplier + spike_events).astype(jnp.float32)


def draw_visual_pos(key, part):
    scores = jax.random.randint(jax.random.fold_in(key, 5), (SECTION_SEQS, N_SEQ, TOK_DEV), 0, 2 ** 30)
    order = jnp.argsort(scores, axis=-1, stable=True)
    return order[:, :, :VSLOT].astype(jnp.int32)


def draw_visual_count(key, part):
    first_key, second_key = jax.random.split(jax.random.fold_in(key, 9), 2)
    counts = jax.random.randint(first_key, (SECTION_SEQS, N_SEQ), CAP, VSLOT + 1)
    full_shard = jax.random.randint(second_key, (SECTION_SEQS,), 0, N_SEQ)
    counts = jnp.where(jnp.arange(N_SEQ)[None, :] == full_shard[:, None], VSLOT, counts)
    return counts.astype(jnp.int32)


def visual_maps(key):
    base = jax.random.fold_in(key, 11)
    key_hot, key_order, key_slot, key_patch = jax.random.split(base, 4)
    hot_owner = jax.random.randint(key_hot, (SECTION_SEQS,), 0, N_SEQ)
    owner_scores = jax.random.randint(key_order, (SECTION_SEQS, N_SEQ, N_SEQ), 0, 2 ** 30)
    owner_ids = jnp.arange(N_SEQ)
    owner_scores = jnp.where(owner_ids[None, None, :] == hot_owner[:, None, None], -1, owner_scores)
    owner_list = jnp.argsort(owner_scores, axis=-1, stable=True)
    slot_ids = jnp.arange(VSLOT)
    slot_scores = jax.random.randint(key_slot, (SECTION_SEQS, N_SEQ, VSLOT), 0, 2 ** 30)
    slot_scores = jnp.where(slot_ids[None, None, :] < CAP, slot_ids[None, None, :] - CAP, slot_scores)
    slot_rank = jnp.argsort(jnp.argsort(slot_scores, axis=-1, stable=True), axis=-1, stable=True)
    owners = jnp.take_along_axis(owner_list, slot_rank // CAP, axis=-1)
    patch_scores = jax.random.randint(key_patch, (SECTION_SEQS, N_SEQ, PATCH_OWN), 0, 2 ** 30)
    patch_perm = jnp.argsort(patch_scores, axis=-1, stable=True)
    column = jnp.arange(N_SEQ)[None, :, None] * CAP + slot_rank % CAP
    micro_ids = jnp.broadcast_to(jnp.arange(SECTION_SEQS)[:, None, None], owners.shape)
    patches = patch_perm[micro_ids, owners, column]
    return (owners.astype(jnp.int32), patches.astype(jnp.int32))


def draw_visual_owner(key, part):
    return visual_maps(key)[0]


def draw_visual_patch(key, part):
    return visual_maps(key)[1]


def levels(own_key, extent, cuts, smallest, high):
    loudness, own = 1.0, jax.random.fold_in(own_key, 6)
    for axis_at, shards_of in cuts:
        heights = jnp.exp(jax.random.uniform(jax.random.fold_in(own, axis_at), (shards_of,), jnp.float32, smallest / len(cuts), high / len(cuts)))
        loudness = loudness * jnp.repeat(heights, extent[axis_at] // shards_of).reshape([-1 if axis == axis_at else 1 for axis in range(len(extent))])
    return loudness


def centred(rng, shape, spread, reach, cuts=(), kind=jnp.bfloat16):
    drawn = spread * jax.random.normal(rng, shape, jnp.float32)
    if cuts:
        drawn = drawn * levels(rng, shape, cuts, -0.22, 0.18)
    return jnp.clip(drawn, -reach, reach).astype(kind)


def setup_inputs(seed: int = 0) -> dict:
    arg_keys = jax.random.split(jax.random.key(seed), 14)
    return {
        "grad_top": centred(arg_keys[0], (SECTION_SEQS, SEQUENCE_TOKENS, D), 1.0, 6.0, ((0, 4), (1, 32))),
        "in_weight": centred(arg_keys[1], (D, HP), D ** -0.5, 0.125, ((0, 128),)),
        "out_weight": centred(arg_keys[2], (D, HP), HP ** -0.5, 0.125, ((0, 128),)),
        "gate_branch": centred(arg_keys[3], (SECTION_SEQS, SEQUENCE_TOKENS, HP), 1.0, 6.0, ((0, 4), (1, 32))),
        "write_vec": centred(arg_keys[4], (SECTION_SEQS, SEQUENCE_TOKENS, N), 0.09, 0.59765625, ((0, 4), (1, 32))),
        "read_vec": centred(arg_keys[5], (SECTION_SEQS, SEQUENCE_TOKENS, N), 1.0, 6.0, ((0, 4), (1, 32))),
        "log_decay": draw_log_decay(jax.random.fold_in(arg_keys[13], 71), 0),
        "step_size": jnp.clip(jnp.exp(math.log(0.05) - 2.3025851 * jax.random.uniform(arg_keys[7], (SECTION_SEQS, LOCAL_HEADS, SEQUENCE_TOKENS), jnp.float32) ** levels(arg_keys[7], (SECTION_SEQS, LOCAL_HEADS, SEQUENCE_TOKENS), ((0, 4), (2, 32)), -0.2, 0.2)), 0.005, 0.05),
        "skip_gain": jnp.clip(jax.random.uniform(arg_keys[8], (LOCAL_HEADS,), jnp.float32, 0.5, 1.5), 0.5, 1.5),
        "visual_pos": draw_visual_pos(jax.random.fold_in(arg_keys[13], 71), 0),
        "visual_count": draw_visual_count(jax.random.fold_in(arg_keys[13], 71), 0),
        "visual_owner": draw_visual_owner(jax.random.fold_in(arg_keys[13], 71), 0),
        "visual_patch": draw_visual_patch(jax.random.fold_in(arg_keys[13], 71), 0),
    }


exact_mode = lax.Precision.HIGHEST


def block_adjoint(inflow, block, skip_row):
    gated, write_rows, read_rows, decay_rows, step_rows = block
    cumulative = jnp.cumsum(decay_rows, axis=1)
    write_f = write_rows.astype(jnp.float32)
    read_f = read_rows.astype(jnp.float32)
    gram = jnp.dot(write_f, read_f.T, precision=exact_mode)
    token_locations = jnp.arange(decay_rows.shape[1])
    causal = token_locations[None, :] >= token_locations[:, None]
    log_gap = cumulative[:, None, :] - cumulative[:, :, None]
    mixing = jnp.where(causal[None], jnp.exp(jnp.minimum(log_gap, 0.0)), 0.0) * gram[None]
    within = jnp.einsum("hts,shp->thp", mixing, gated, precision=exact_mode)
    tail_decay = jnp.exp(cumulative[:, -1:] - cumulative).T
    from_later = jnp.einsum("hpn,tn->thp", inflow, write_f, precision=exact_mode) * tail_decay[:, :, None]
    inner_grad = step_rows.T[:, :, None] * (within + from_later) + skip_row[None, :, None] * gated
    scaled = gated * jnp.exp(cumulative).T[:, :, None]
    contrib = jnp.einsum("shp,sn->hpn", scaled, read_f, precision=exact_mode)
    outflow = contrib + jnp.exp(cumulative[:, -1])[:, None, None] * inflow
    return outflow, inner_grad


def ssd_adjoint(gated, write_rows, read_rows, decay_rows, step_rows, skip_row):
    blk = min(GROUP, TOK_DEV)
    count = SEQUENCE_TOKENS // blk
    gated_blocks = gated.reshape(count, blk, LOCAL_HEADS, P_SIZE)
    write_blocks = write_rows.reshape(count, blk, N)
    read_blocks = read_rows.reshape(count, blk, N)
    decay_blocks = decay_rows.reshape(LOCAL_HEADS, count, blk).transpose(1, 0, 2)
    step_blocks = step_rows.reshape(LOCAL_HEADS, count, blk).transpose(1, 0, 2)
    start = jnp.zeros((LOCAL_HEADS, P_SIZE, N), jnp.float32)

    def advance(inflow, block):
        return block_adjoint(inflow, block, skip_row)

    _, inner_grad = lax.scan(advance, start, (gated_blocks, write_blocks, read_blocks, decay_blocks, step_blocks), reverse=True)
    return inner_grad.reshape(SEQUENCE_TOKENS, LOCAL_HEADS * P_SIZE)


def layer_back(incoming, w_in, w_out, gate_val, write_rows, read_rows, decay_rows, step_rows, skip_row):
    gated = jnp.dot(incoming, w_out, preferred_element_type=jnp.float32) * jax.nn.silu(gate_val.astype(jnp.float32))
    inner_grad = ssd_adjoint(gated.reshape(SEQUENCE_TOKENS, LOCAL_HEADS, P_SIZE), write_rows, read_rows, decay_rows, step_rows, skip_row)
    inner_grad = inner_grad.astype(jnp.bfloat16)
    back = lax.dot_general(inner_grad, w_in, (((1,), (1,)), ((), ())), preferred_element_type=jnp.float32)
    return (incoming.astype(jnp.float32) + back).astype(jnp.bfloat16)


def reference(grad_top, in_weight, out_weight, gate_branch, write_vec, read_vec, log_decay, step_size, skip_gain, visual_pos, visual_count, visual_owner, visual_patch):
    results = []
    for micro in range(SECTION_SEQS):
        results.append(layer_back(grad_top[micro], in_weight, out_weight, gate_branch[micro], write_vec[micro], read_vec[micro], log_decay[micro], step_size[micro], skip_gain))
    layer_grads = jnp.stack(results)
    tables = []
    for micro in range(SECTION_SEQS):
        shard_rows = layer_grads[micro].reshape(N_SEQ, TOK_DEV, D)
        picked = jax.vmap(lambda frame_rows, positions: frame_rows[positions])(shard_rows, visual_pos[micro])
        live_slot = jnp.arange(VSLOT)[None, :] < visual_count[micro][:, None]
        target = (visual_owner[micro] * PATCH_OWN + visual_patch[micro]).reshape(-1)
        values = jnp.where(live_slot[:, :, None], picked.astype(jnp.float32), 0.0).reshape(N_SEQ * VSLOT, D)
        table = jnp.zeros((N_SEQ * PATCH_OWN, D), jnp.float32).at[target].add(values)
        tables.append(table.astype(jnp.bfloat16))
    return layer_grads, jnp.stack(tables)
```

```python
import functools
import jax
import jax.numpy as jnp
import numpy as np
from jax import lax
from jax.experimental import pallas as pl
from jax.experimental.pallas import tpu as pltpu
from jax.sharding import Mesh
from jax.sharding import PartitionSpec as P

BLK = 256
CAP = 2
X, Z, C, Y = ("seq_0", "seq_1", "seq_2", "section")
SEQ = (X, Z, C)
ALL = (X, Z, C, Y)
SIZES = (4, 4, 2, 4)
HG = 4


def ring_perm(axis, shift):
    at = ALL.index(axis)
    pairs = []
    for i in range(int(np.prod(SIZES))):
        where = list(np.unravel_index(i, SIZES))
        sign = 1 if where[2] == 0 else -1
        where[at] = (where[at] + sign * shift) % SIZES[at]
        pairs.append((i, int(np.ravel_multi_index(where, SIZES))))
    return pairs


def send(a, axis, shift):
    return lax.ppermute(a, ALL, ring_perm(axis, shift))


def swap_cores(a):
    return lax.ppermute(a, C, [(0, 1), (1, 0)])


def chip_rows(own, other, core, axis=0):
    first = core == 0
    return jnp.concatenate([jnp.where(first, own, other), jnp.where(first, other, own)], axis=axis)


def half_of(a, which, axis):
    width = a.shape[axis] // 2
    return lax.dynamic_slice_in_dim(a, which * width, width, axis)


def factors_kernel(write_ref, read_ref, read_t_ref, row_ref, col_ref, step_ref, mix_ref, rt_ref, wt_ref):
    write = write_ref[...]
    read = read_ref[...]
    gram = lax.dot_general(write, read, (((1,), (1,)), ((), ())), preferred_element_type=jnp.float32)
    write_f = write.astype(jnp.float32)
    read_t = read_t_ref[...].astype(jnp.float32)
    t = lax.broadcasted_iota(jnp.int32, gram.shape, 0)
    s = lax.broadcasted_iota(jnp.int32, gram.shape, 1)
    gram = jnp.where(s >= t, gram, 0.0)
    for h in range(HG):
        row = row_ref[0, 0, h : h + 1, :]
        col = col_ref[0, 0, :, h : h + 1]
        step = step_ref[0, 0, :, h : h + 1]
        decay = jnp.exp(jnp.minimum(row - col, 0.0))
        mix_ref[0, h] = (decay * (gram * step)).astype(jnp.bfloat16)
        rt_ref[0, h] = (read_t * jnp.exp(row)).astype(jnp.bfloat16)
        last = row[:, row.shape[1] - 1 :]
        wt_ref[0, h] = (write_f * (jnp.exp(last - col) * step)).astype(jnp.bfloat16)


def factors(write, read, cum, step):
    heads, blocks, _ = cum.shape
    groups = heads // HG
    n = write.shape[1]
    row = cum.reshape(groups, HG, blocks, BLK).transpose(2, 0, 1, 3)
    col = row.transpose(0, 1, 3, 2)
    step_col = step.reshape(groups, HG, blocks, BLK).transpose(2, 0, 3, 1)
    col_spec = pl.BlockSpec((1, 1, BLK, HG), lambda b, g: (b, g, 0, 0))
    return pl.pallas_call(
        factors_kernel,
        grid=(blocks, groups),
        in_specs=[
            pl.BlockSpec((BLK, n), lambda b, g: (b, 0)),
            pl.BlockSpec((BLK, n), lambda b, g: (b, 0)),
            pl.BlockSpec((n, BLK), lambda b, g: (0, b)),
            pl.BlockSpec((1, 1, HG, BLK), lambda b, g: (b, g, 0, 0)),
            col_spec,
            col_spec,
        ],
        out_specs=[
            pl.BlockSpec((1, HG, BLK, BLK), lambda b, g: (b, g, 0, 0)),
            pl.BlockSpec((1, HG, n, BLK), lambda b, g: (b, g, 0, 0)),
            pl.BlockSpec((1, HG, BLK, n), lambda b, g: (b, g, 0, 0)),
        ],
        out_shape=[
            jax.ShapeDtypeStruct((blocks, heads, BLK, BLK), jnp.bfloat16),
            jax.ShapeDtypeStruct((blocks, heads, n, BLK), jnp.bfloat16),
            jax.ShapeDtypeStruct((blocks, heads, BLK, n), jnp.bfloat16),
        ],
        compiler_params=pltpu.CompilerParams(dimension_semantics=("arbitrary", "arbitrary")),
        cost_estimate=pl.CostEstimate(flops=5 * 10**9, bytes_accessed=22 * 10**6, transcendentals=10**7),
        name="factors",
    )(write, read, read.T, row, col, step_col)


def gated_kernel(place_ref, *refs):
    pieces, (x_ref, gate_ref, rt_ref, total_ref, g_ref, local_ref, state_ref, w_ref, sem) = refs[:8], refs[8:]
    step = pl.program_id(0)
    rows, width = pieces[0].shape[1:]
    pairs = state_ref.shape[0]

    def copies():
        for color in range(2):
            for k2 in range(4):
                for k1 in range(4):
                    at = pl.multiple_of(place_ref[color * 16 + k2 * 4 + k1] * rows, 16)
                    yield pltpu.make_async_copy(
                        pieces[color * 4 + k2].at[k1],
                        w_ref.at[pl.ds(at, rows), pl.ds(color * width, width)],
                        sem.at[color * 16 + k2 * 4 + k1],
                    )

    @pl.when(step == 0)
    def _():
        for copy in copies():
            copy.start()
        state_ref[...] = jnp.zeros_like(state_ref)
        for copy in copies():
            copy.wait()

    value = jnp.dot(x_ref[...], w_ref[...], preferred_element_type=jnp.float32)
    gate = gate_ref[...].astype(jnp.float32)
    gated = (value * (gate / (1.0 + jnp.exp(-gate)))).astype(jnp.bfloat16)
    g_ref[...] = gated
    for p in range(pairs):
        cols = slice(p * 128, (p + 1) * 128)
        low = jnp.dot(rt_ref[0, 2 * p], gated[:, cols], preferred_element_type=jnp.float32)
        high = jnp.dot(rt_ref[0, 2 * p + 1], gated[:, cols], preferred_element_type=jnp.float32)
        lane = lax.broadcasted_iota(jnp.int32, low.shape, 1)
        added = jnp.where(lane < 64, low, high)
        later = state_ref[p]
        local_ref[0, p] = later
        state_ref[p] = added + total_ref[0, :, cols] * later


def gated_and_states(place, pieces, x, gate, rt, total):
    tokens, depth = x.shape
    width = gate.shape[1]
    blocks = tokens // BLK
    pairs = width // 128
    n = rt.shape[2]
    back = lambda i: blocks - 1 - i
    return pl.pallas_call(
        gated_kernel,
        grid_spec=pltpu.PrefetchScalarGridSpec(
            num_scalar_prefetch=1,
            grid=(blocks,),
            in_specs=[pl.BlockSpec(memory_space=pl.ANY)] * 8
            + [
                pl.BlockSpec((BLK, depth), lambda i, s: (back(i), 0)),
                pl.BlockSpec((BLK, width), lambda i, s: (back(i), 0)),
                pl.BlockSpec((1, 2 * pairs, n, BLK), lambda i, s: (back(i), 0, 0, 0)),
                pl.BlockSpec((1, 1, width), lambda i, s: (back(i), 0, 0)),
            ],
            out_specs=[
                pl.BlockSpec((BLK, width), lambda i, s: (back(i), 0)),
                pl.BlockSpec((1, pairs, n, 128), lambda i, s: (back(i), 0, 0, 0)),
                pl.BlockSpec((pairs, n, 128), lambda i, s: (0, 0, 0)),
            ],
            scratch_shapes=[pltpu.VMEM((depth, width), jnp.bfloat16), pltpu.SemaphoreType.DMA((32,))],
        ),
        out_shape=[
            jax.ShapeDtypeStruct((tokens, width), jnp.bfloat16),
            jax.ShapeDtypeStruct((blocks, pairs, n, 128), jnp.float32),
            jax.ShapeDtypeStruct((pairs, n, 128), jnp.float32),
        ],
        compiler_params=pltpu.CompilerParams(
            dimension_semantics=("arbitrary",), vmem_limit_bytes=50 * 2**20
        ),
        cost_estimate=pl.CostEstimate(flops=8 * 10**9, bytes_accessed=24 * 10**6, transcendentals=2 * 10**6),
        name="gated",
    )(place, *pieces, x, gate, rt, total)


def inner_kernel(mix_ref, wt_ref, g_ref, local_ref, inflow_ref, coef_ref, skip_ref, out_ref):
    for p in range(HG // 2):
        cols = slice(p * 128, (p + 1) * 128)
        g = g_ref[:, cols]
        arriving = local_ref[0, p] + coef_ref[0, :, cols] * inflow_ref[p].astype(jnp.float32)
        arriving = arriving.astype(jnp.bfloat16)
        halves = []
        for h in (2 * p, 2 * p + 1):
            halves.append(
                jnp.dot(mix_ref[0, h], g, preferred_element_type=jnp.float32)
                + jnp.dot(wt_ref[0, h], arriving, preferred_element_type=jnp.float32)
            )
        lane = lax.broadcasted_iota(jnp.int32, halves[0].shape, 1)
        own = jnp.where(lane < 64, halves[0], halves[1])
        out_ref[:, cols] = (own + skip_ref[:, cols] * g.astype(jnp.float32)).astype(jnp.bfloat16)


def inner_gradient(mix, wt, gated, local, inflow, coef, skip):
    tokens, width = gated.shape
    blocks, heads = mix.shape[:2]
    n = wt.shape[3]
    groups = heads // HG
    return pl.pallas_call(
        inner_kernel,
        grid=(blocks, groups),
        in_specs=[
            pl.BlockSpec((1, HG, BLK, BLK), lambda b, g: (b, g, 0, 0)),
            pl.BlockSpec((1, HG, BLK, n), lambda b, g: (b, g, 0, 0)),
            pl.BlockSpec((BLK, HG * 64), lambda b, g: (b, g)),
            pl.BlockSpec((1, HG // 2, n, 128), lambda b, g: (b, g, 0, 0)),
            pl.BlockSpec((HG // 2, n, 128), lambda b, g: (g, 0, 0)),
            pl.BlockSpec((1, 1, HG * 64), lambda b, g: (b, 0, g)),
            pl.BlockSpec((1, HG * 64), lambda b, g: (0, g)),
        ],
        out_specs=pl.BlockSpec((BLK, HG * 64), lambda b, g: (b, g)),
        out_shape=jax.ShapeDtypeStruct((tokens, width), jnp.bfloat16),
        compiler_params=pltpu.CompilerParams(dimension_semantics=("arbitrary", "arbitrary")),
        cost_estimate=pl.CostEstimate(flops=6 * 10**9, bytes_accessed=25 * 10**6, transcendentals=0),
        name="inner",
    )(mix, wt, gated, local, inflow, coef, skip)


def body(
    grad_top,
    in_weight,
    out_weight,
    gate_branch,
    write_vec,
    read_vec,
    log_decay,
    step_size,
    skip_gain,
    visual_pos,
    visual_count,
    visual_owner,
    visual_patch,
):
    x_at, z_at, core = lax.axis_index(X), lax.axis_index(Z), lax.axis_index(C)
    seq_count = lax.axis_size(SEQ)
    seq_index = lax.axis_index(SEQ)
    chips = lax.axis_size(X) * lax.axis_size(Z)
    chip = x_at * lax.axis_size(Z) + z_at
    sign = 1 - 2 * core
    grad_rows = grad_top[0]
    tok_rows, model_width = grad_rows.shape

    rows_y = lax.all_gather(jnp.concatenate([out_weight, in_weight], axis=1), Y, axis=0, tiled=True)
    w_out_rows, w_in_rows = rows_y[:, : out_weight.shape[1]], rows_y[:, out_weight.shape[1] :]
    w_in_full = lax.all_gather(w_in_rows, SEQ, axis=0, tiled=True)

    w_mine = half_of(w_out_rows, core, 1)
    w_other = swap_cores(half_of(w_out_rows, 1 - core, 1))
    w_chip = chip_rows(w_mine, w_other, core)
    part = w_chip.shape[1] // 2
    pieces = []
    places = []
    for color, (first, second) in enumerate(((X, Z), (Z, X))):
        own = w_chip[:, color * part : (color + 1) * part]
        plane = jnp.stack([own] + [send(own, first, s) for s in (1, 2, 3)])
        for k2 in range(4):
            pieces.append(plane)
            if k2 < 3:
                plane = send(plane, second, 1)
            for k1 in range(4):
                kx, kz = (k1, k2) if color == 0 else (k2, k1)
                places.append(lax.rem(x_at - sign * kx + 4, 4) * 4 + lax.rem(z_at - sign * kz + 4, 4))
    place = jnp.stack(places).astype(jnp.int32)

    x_chip = chip_rows(grad_rows, swap_cores(grad_rows), core)
    gate_chip = chip_rows(
        half_of(gate_branch[0], core, 1), swap_cores(half_of(gate_branch[0], 1 - core, 1)), core
    )
    vectors = jnp.concatenate([write_vec[0], read_vec[0]], axis=1)
    vectors = chip_rows(vectors, swap_cores(vectors), core)
    n = write_vec.shape[2]
    write, read = vectors[:, :n], vectors[:, n:]
    scalars = jnp.stack([log_decay[0], step_size[0]])
    scalars = chip_rows(half_of(scalars, core, 1), swap_cores(half_of(scalars, 1 - core, 1)), core, axis=2)
    heads = scalars.shape[1]
    blocks = scalars.shape[2] // BLK
    decay, step = scalars.reshape(2, heads, blocks, BLK)
    skip = jnp.repeat(half_of(skip_gain, core, 0), 64)[None]

    cum = jnp.cumsum(decay, axis=2)
    tot = jnp.sum(decay, axis=2)
    lanes = lambda a: jnp.repeat(a, 64, axis=0).T[:, None, :]
    after = jnp.cumsum(tot[:, ::-1], axis=1)[:, ::-1] - tot
    chip_tot = jnp.sum(tot, axis=1)
    all_tot = lax.all_gather(chip_tot, (X, Z), axis=0)
    pairs = heads // 2
    chunk = pairs * n // chips
    mine = (chip * chunk + jnp.arange(chunk)) // n
    chunk_decay = jnp.exp(jnp.repeat(all_tot, 64, axis=1)).reshape(chips, pairs, 128)[:, mine]

    mix, rt, wt = factors(write, read, cum, step)
    gated, local, state = gated_and_states(place, pieces, x_chip, gate_chip, rt, jnp.exp(lanes(tot)))

    share = lax.all_to_all(
        state.astype(jnp.bfloat16).reshape(chips, chunk, 128), (X, Z), 0, 0, tiled=True
    ).astype(jnp.float32)
    run = jnp.zeros((chunk, 128), jnp.float32)
    outs = [None] * chips
    for q in reversed(range(chips)):
        outs[q] = run.astype(jnp.bfloat16)
        run = share[q] + chunk_decay[q] * run
    inflow = lax.all_to_all(jnp.stack(outs), (X, Z), 0, 0, tiled=True).reshape(pairs, n, 128)

    inner_chip = inner_gradient(mix, wt, gated, local, inflow, jnp.exp(lanes(after)), skip)
    inner_mine = half_of(inner_chip, core, 0)
    inner_other = swap_cores(half_of(inner_chip, 1 - core, 0))
    inner = chip_rows(inner_mine, inner_other, core, axis=1)

    owner_row = visual_owner[0]
    patch_row = visual_patch[0]
    count_row = visual_count[0]
    slot_count = owner_row.shape[1]
    slot_ids = jnp.arange(slot_count)
    live_slot = slot_ids[None, :] < count_row[:, None]
    earlier_slot = slot_ids[None, :] < slot_ids[:, None]
    same_owner = (
        (owner_row[:, :, None] == owner_row[:, None, :])
        & live_slot[:, None, :]
        & earlier_slot[None]
    )
    rank_row = jnp.sum(same_owner.astype(jnp.int32), axis=2)
    own_owner = lax.dynamic_index_in_dim(owner_row, seq_index, 0, keepdims=False)
    own_rank = lax.dynamic_index_in_dim(rank_row, seq_index, 0, keepdims=False)
    own_live = lax.dynamic_index_in_dim(live_slot, seq_index, 0, keepdims=False)
    destination = own_owner * CAP + own_rank
    send_columns = jnp.arange(seq_count * CAP)
    send_map = ((send_columns[:, None] == destination[None, :]) & own_live[None, :]).astype(jnp.bfloat16)
    pos_map = (visual_pos[0, 0][:, None] == jnp.arange(tok_rows)[None, :]).astype(jnp.bfloat16)
    take = jnp.dot(send_map, pos_map, preferred_element_type=jnp.float32).astype(jnp.bfloat16)

    def exchange(rows):
        sent = jnp.dot(take, rows, preferred_element_type=jnp.float32).astype(jnp.bfloat16)
        sent = sent.reshape(seq_count, CAP, rows.shape[1])
        return lax.all_to_all(sent, SEQ, 0, 0, tiled=True).reshape(seq_count * CAP, rows.shape[1])

    mine_mask = live_slot & (owner_row == seq_index)
    column = jnp.arange(seq_count)[:, None] * CAP + rank_row
    patch_count = seq_count * CAP
    patch_hit = (
        (patch_row.reshape(-1)[:, None] == jnp.arange(patch_count)[None, :])
        & mine_mask.reshape(-1)[:, None]
    ).astype(jnp.bfloat16)
    column_hit = (column.reshape(-1)[:, None] == send_columns[None, :]).astype(jnp.bfloat16)
    select = lax.dot_general(
        patch_hit, column_hit, (((0,), (0,)), ((), ())), preferred_element_type=jnp.float32
    ).astype(jnp.bfloat16)
    placed = lambda rows: jnp.dot(select, rows, preferred_element_type=jnp.float32)

    def project(rows, base):
        back = lax.dot_general(rows, w_in_full, (((1,), (1,)), ((), ())), preferred_element_type=jnp.float32)
        return (base.astype(jnp.float32) + back).astype(jnp.bfloat16)

    grad_patches = placed(exchange(grad_rows))
    inner_patches = placed(exchange(inner)).astype(jnp.bfloat16)
    result = project(inner, grad_rows)
    patches = project(inner_patches, grad_patches)
    return (result[None], patches[None])


def solution(mesh):
    finer = Mesh(mesh.devices.reshape(SIZES), ALL)
    return jax.shard_map(
        body,
        mesh=finer,
        in_specs=(
            P(Y, SEQ, None),
            P(ALL, None),
            P(ALL, None),
            P(Y, SEQ, None),
            P(Y, SEQ, None),
            P(Y, SEQ, None),
            P(Y, None, SEQ),
            P(Y, None, SEQ),
            P(),
            P(Y, SEQ, None),
            P(Y, None),
            P(Y, None, None),
            P(Y, None, None),
        ),
        out_specs=(P(Y, SEQ, None), P(Y, SEQ, None)),
        check_vma=False,
    )
```

```python
import functools
import jax
import jax.numpy as jnp
import numpy as np
from jax import lax
from jax.experimental import pallas as pl
from jax.experimental.pallas import tpu as pltpu
from jax.sharding import Mesh
from jax.sharding import PartitionSpec as P

BLK = 128
MID = 63
STEP = 256
CAP = 2
X, Z, C, Y = ("seq_0", "seq_1", "seq_2", "section")
SEQ = (X, Z, C)
ALL = (X, Z, C, Y)
SIZES = (4, 4, 2, 4)


def ring_perm(axis, shift):
    at = ALL.index(axis)
    pairs = []
    for i in range(int(np.prod(SIZES))):
        where = list(np.unravel_index(i, SIZES))
        sign = 1 if where[2] == 0 else -1
        where[at] = (where[at] + sign * shift) % SIZES[at]
        pairs.append((i, int(np.ravel_multi_index(where, SIZES))))
    return pairs


def send(a, axis, shift):
    return lax.ppermute(a, ALL, ring_perm(axis, shift))


def swap_cores(a):
    return lax.ppermute(a, C, [(0, 1), (1, 0)])


def chip_rows(own, other, core, axis=0):
    first = core == 0
    return jnp.concatenate([jnp.where(first, own, other), jnp.where(first, other, own)], axis=axis)


def half_of(a, which, axis):
    width = a.shape[axis] // 2
    return lax.dynamic_slice_in_dim(a, which * width, width, axis)


def split(a):
    high = a.astype(jnp.bfloat16).astype(jnp.float32)
    return jnp.concatenate([high, a - high], axis=0).astype(jnp.bfloat16)


def spread(parts, heads_ref):
    return lax.dot_general(
        parts, heads_ref[...], (((0,), (0,)), ((), ())), preferred_element_type=jnp.float32
    )


def decays_kernel(info_ref, decay_ref, step_ref, other_ref, heads_ref, u_ref, v_ref, row_ref, extra_ref):
    heads = decay_ref.shape[0] // 2
    core = info_ref[0]
    first = core == 0
    own_decay = jnp.where(first, decay_ref[:heads], decay_ref[heads:])
    own_step = jnp.where(first, step_ref[:heads], step_ref[heads:])
    blocks = v_ref.shape[0]
    per = blocks // 2
    r = lax.broadcasted_iota(jnp.int32, (BLK, BLK), 0)
    c = lax.broadcasted_iota(jnp.int32, (BLK, BLK), 1)
    tri = (r <= c).astype(jnp.float32)
    lane = lax.broadcasted_iota(jnp.int32, (heads, BLK), 1)
    after = jnp.zeros((heads, 1), jnp.float32)
    for b in reversed(range(blocks)):
        cols = slice((b % per) * BLK, (b % per + 1) * BLK)
        own = core == b // per
        decay = jnp.where(own, own_decay[:, cols], other_ref[:heads, cols])
        step = jnp.where(own, own_step[:, cols], other_ref[heads:, cols])
        cum = jnp.dot(decay, tri, precision=lax.Precision.HIGHEST, preferred_element_type=jnp.float32)
        mid = cum[:, MID : MID + 1]
        tot = cum[:, BLK - 1 :]
        v_ref[b] = split(jnp.exp(cum - mid))
        u_ref[b] = split(jnp.exp(mid - cum) * step)
        rows = jnp.where(
            lane == 0,
            jnp.exp(mid),
            jnp.where(
                lane == 1,
                jnp.exp(tot),
                jnp.where(lane == 2, jnp.exp(tot - mid), jnp.exp(tot - mid) * jnp.exp(after)),
            ),
        )
        row_ref[b] = spread(split(rows), heads_ref)[:8]
        after = after + tot
    eye = lax.broadcasted_iota(jnp.int32, (heads, BLK), 0) == lane
    whole = jnp.sum(jnp.where(eye, jnp.exp(after), 0.0), axis=0, keepdims=True)
    high = whole.astype(jnp.bfloat16).astype(jnp.float32)
    row = lax.broadcasted_iota(jnp.int32, (8, BLK), 0)
    extra_ref[...] = jnp.where(row == 0, high, jnp.where(row == 1, whole - high, 0.0)).astype(jnp.bfloat16)


def decays(info, decay, step, other, heads_map):
    heads = decay.shape[0] // 2
    blocks = 2 * decay.shape[1] // BLK
    vmem = pl.BlockSpec(memory_space=pltpu.VMEM)
    return pl.pallas_call(
        decays_kernel,
        in_specs=[pl.BlockSpec(memory_space=pltpu.SMEM)] + [vmem] * 4,
        out_specs=[vmem] * 4,
        out_shape=[
            jax.ShapeDtypeStruct((blocks, 2 * heads, BLK), jnp.bfloat16),
            jax.ShapeDtypeStruct((blocks, 2 * heads, BLK), jnp.bfloat16),
            jax.ShapeDtypeStruct((blocks, 8, heads_map.shape[1]), jnp.float32),
            jax.ShapeDtypeStruct((8, BLK), jnp.bfloat16),
        ],
        cost_estimate=pl.CostEstimate(flops=10**9, bytes_accessed=10**6, transcendentals=10**5),
        name="decays",
    )(info, decay, step, other, heads_map)


def gated_kernel(info_ref, place_ref, *refs):
    pieces = refs[:8]
    (x_own_ref, x_other_ref, gate_own_ref, gate_other_ref, read_ref, v_ref, row_ref, extra_ref, heads_ref,
     g_ref, gv_ref, local_ref, share_ref, state_ref, w_ref, sem) = refs[8:]
    step = pl.program_id(0)
    core = info_ref[0]
    rows, part = pieces[0].shape[1:]

    def copies():
        for color in range(2):
            for k2 in range(4):
                for k1 in range(4):
                    at = pl.multiple_of(place_ref[color * 16 + k2 * 4 + k1] * rows, 16)
                    yield pltpu.make_async_copy(
                        pieces[color * 4 + k2].at[k1],
                        w_ref.at[pl.ds(at, rows), pl.ds(color * part, part)],
                        sem.at[color * 16 + k2 * 4 + k1],
                    )

    @pl.when(step == 0)
    def _():
        for copy in copies():
            copy.start()
        state_ref[...] = jnp.zeros_like(state_ref)
        for copy in copies():
            copy.wait()

    block = pl.num_programs(0) - 1 - step
    own = (block // 2) == core
    x = jnp.where(own, x_own_ref[...], x_other_ref[...])
    value = jnp.dot(x, w_ref[...], preferred_element_type=jnp.float32)
    gate = jnp.where(own, gate_own_ref[...], gate_other_ref[...]).astype(jnp.float32)
    gated = value * (gate / (1.0 + jnp.exp(-gate)))
    g_ref[...] = gated.astype(jnp.bfloat16)
    for b in reversed(range(STEP // BLK)):
        at = slice(b * BLK, (b + 1) * BLK)
        gv = (gated[at] * spread(v_ref[b], heads_ref)).astype(jnp.bfloat16)
        gv_ref[at] = gv
        added = lax.dot_general(
            read_ref[at], gv, (((0,), (0,)), ((), ())), preferred_element_type=jnp.float32
        )
        later = state_ref[...]
        local_ref[b] = (later * row_ref[b, 2:3]).astype(jnp.bfloat16)
        state_ref[...] = added * row_ref[b, 0:1] + row_ref[b, 1:2] * later

    @pl.when(step == pl.num_programs(0) - 1)
    def _():
        width = state_ref.shape[1]
        for j in range(share_ref.shape[0]):
            share_ref[j, :, :width] = state_ref[j * 8 : (j + 1) * 8].astype(jnp.bfloat16)
            share_ref[j, :, width:] = extra_ref[...]


def gated_and_states(info, place, pieces, x_own, x_other, gate_own, gate_other, read, v, row, extra, heads_map):
    depth = x_own.shape[1]
    width = gate_other.shape[1]
    blocks = v.shape[0]
    n = read.shape[1]
    steps = blocks * BLK // STEP
    per = STEP // BLK
    tokens = blocks * BLK
    chips = n // 8
    back = lambda i: steps - 1 - i

    def own_at(i, s):
        return jnp.where(s[0] == 1, jnp.maximum(1 - i, 0), jnp.minimum(1, steps - 1 - i))

    def other_at(i, s):
        return jnp.where(s[0] == 0, jnp.maximum(1 - i, 0), jnp.minimum(1, steps - 1 - i))

    return pl.pallas_call(
        gated_kernel,
        grid_spec=pltpu.PrefetchScalarGridSpec(
            num_scalar_prefetch=2,
            grid=(steps,),
            in_specs=[pl.BlockSpec(memory_space=pl.ANY)] * 8
            + [
                pl.BlockSpec((STEP, depth), lambda i, s, t: (own_at(i, s), 0)),
                pl.BlockSpec((STEP, depth), lambda i, s, t: (other_at(i, s), 0)),
                pl.BlockSpec((STEP, width), lambda i, s, t: (own_at(i, s), s[0])),
                pl.BlockSpec((STEP, width), lambda i, s, t: (other_at(i, s), 0)),
                pl.BlockSpec((STEP, n), lambda i, s, t: (back(i), 0)),
                pl.BlockSpec((per, *v.shape[1:]), lambda i, s, t: (back(i), 0, 0)),
                pl.BlockSpec((per, 8, width), lambda i, s, t: (back(i), 0, 0)),
                pl.BlockSpec(extra.shape, lambda i, s, t: (0, 0)),
                pl.BlockSpec(heads_map.shape, lambda i, s, t: (0, 0)),
            ],
            out_specs=[
                pl.BlockSpec((STEP, width), lambda i, s, t: (back(i), 0)),
                pl.BlockSpec((STEP, width), lambda i, s, t: (back(i), 0)),
                pl.BlockSpec((per, n, width), lambda i, s, t: (back(i), 0, 0)),
                pl.BlockSpec((chips, 8, width + BLK), lambda i, s, t: (0, 0, 0)),
            ],
            scratch_shapes=[
                pltpu.VMEM((n, width), jnp.float32),
                pltpu.VMEM((depth, width), jnp.bfloat16),
                pltpu.SemaphoreType.DMA((32,)),
            ],
        ),
        out_shape=[
            jax.ShapeDtypeStruct((tokens, width), jnp.bfloat16),
            jax.ShapeDtypeStruct((tokens, width), jnp.bfloat16),
            jax.ShapeDtypeStruct((blocks, n, width), jnp.bfloat16),
            jax.ShapeDtypeStruct((chips, 8, width + BLK), jnp.bfloat16),
        ],
        compiler_params=pltpu.CompilerParams(
            dimension_semantics=("arbitrary",), vmem_limit_bytes=50 * 2**20
        ),
        cost_estimate=pl.CostEstimate(flops=8 * 10**9, bytes_accessed=24 * 10**6, transcendentals=2 * 10**6),
        name="gated",
    )(info, place, *pieces, x_own, x_other, gate_own, gate_other, read, v, row, extra, heads_map)


def suffix_kernel(share_ref, heads_ref, out_ref):
    chips, _, width = out_ref.shape
    heads = heads_ref.shape[0] // 2
    parts = share_ref[:, 0:1, width:].reshape(chips, BLK), share_ref[:, 1:2, width:].reshape(chips, BLK)
    spread_of = lambda a: jnp.dot(a[:, :heads], heads_ref[:heads], preferred_element_type=jnp.float32)
    decay = spread_of(parts[0]) + spread_of(parts[1])
    run = jnp.zeros(out_ref.shape[1:], jnp.float32)
    for q in reversed(range(chips)):
        out_ref[q] = run.astype(jnp.bfloat16)
        run = share_ref[q, :, :width].astype(jnp.float32) + decay[q : q + 1] * run


def suffix(share, heads_map):
    chips, rows, _ = share.shape
    vmem = pl.BlockSpec(memory_space=pltpu.VMEM)
    return pl.pallas_call(
        suffix_kernel,
        in_specs=[vmem, vmem],
        out_specs=vmem,
        out_shape=jax.ShapeDtypeStruct((chips, rows, heads_map.shape[1]), jnp.bfloat16),
        cost_estimate=pl.CostEstimate(flops=10**8, bytes_accessed=10**6, transcendentals=0),
        name="suffix",
    )(share, heads_map)


def inner_kernel(
    info_ref, write_ref, read_ref, u_ref, g_ref, gv_ref, local_ref, inflow_ref, row_ref, skip_ref, heads_ref, out_ref
):
    r = lax.broadcasted_iota(jnp.int32, (BLK, BLK), 0)
    c = lax.broadcasted_iota(jnp.int32, (BLK, BLK), 1)
    for b in range(STEP // BLK):
        at = slice(b * BLK, (b + 1) * BLK)
        write = write_ref[at]
        gram = lax.dot_general(
            write, read_ref[at], (((1,), (1,)), ((), ())), preferred_element_type=jnp.float32
        )
        left = jnp.concatenate([jnp.where(c >= r, gram, 0.0).astype(jnp.bfloat16), write], axis=1)
        arriving = local_ref[b].astype(jnp.float32) + row_ref[b, 3:4] * inflow_ref[...].astype(jnp.float32)
        right = jnp.concatenate([gv_ref[at], arriving.astype(jnp.bfloat16)], axis=0)
        value = jnp.dot(left, right, preferred_element_type=jnp.float32) * spread(u_ref[b], heads_ref)
        out_ref[at] = (value + skip_ref[...] * g_ref[at].astype(jnp.float32)).astype(jnp.bfloat16)


def inner_gradient(info, write, read, u, gated, gated_v, local, inflow, row, skip, heads_map, own):
    tokens, width = gated.shape
    n = write.shape[1]
    per = STEP // BLK
    steps = tokens // STEP // 2
    at = (lambda i, s: s[0] * steps + i) if own else (lambda i, s: (1 - s[0]) * steps + i)
    return pl.pallas_call(
        inner_kernel,
        grid_spec=pltpu.PrefetchScalarGridSpec(
            num_scalar_prefetch=1,
            grid=(steps,),
            in_specs=[
                pl.BlockSpec((STEP, n), lambda i, s: (at(i, s), 0)),
                pl.BlockSpec((STEP, n), lambda i, s: (at(i, s), 0)),
                pl.BlockSpec((per, *u.shape[1:]), lambda i, s: (at(i, s), 0, 0)),
                pl.BlockSpec((STEP, width), lambda i, s: (at(i, s), 0)),
                pl.BlockSpec((STEP, width), lambda i, s: (at(i, s), 0)),
                pl.BlockSpec((per, n, width), lambda i, s: (at(i, s), 0, 0)),
                pl.BlockSpec((n, width), lambda i, s: (0, 0)),
                pl.BlockSpec((per, 8, width), lambda i, s: (at(i, s), 0, 0)),
                pl.BlockSpec((1, width), lambda i, s: (0, 0)),
                pl.BlockSpec(heads_map.shape, lambda i, s: (0, 0)),
            ],
            out_specs=pl.BlockSpec((STEP, width), lambda i, s: (i, 0)),
        ),
        out_shape=jax.ShapeDtypeStruct((tokens // 2, width), jnp.bfloat16),
        compiler_params=pltpu.CompilerParams(
            dimension_semantics=("arbitrary",), vmem_limit_bytes=40 * 2**20
        ),
        cost_estimate=pl.CostEstimate(flops=10**9, bytes_accessed=6 * 10**6, transcendentals=0),
        name="inner_own" if own else "inner_other",
    )(info, write, read, u, gated, gated_v, local, inflow, row, skip, heads_map)


def product_kernel(info_ref, own_ref, other_ref, w_ref, base_ref, out_ref, lhs_ref):
    core = info_ref[0]
    width = own_ref.shape[1]

    @pl.when(pl.program_id(0) == 0)
    def _():
        lhs_ref[:, pl.ds(pl.multiple_of(core * width, 128), width)] = own_ref[...]
        lhs_ref[:, pl.ds(pl.multiple_of((1 - core) * width, 128), width)] = other_ref[...]

    value = lax.dot_general(
        lhs_ref[...], w_ref[...], (((1,), (1,)), ((), ())), preferred_element_type=jnp.float32
    )
    out_ref[...] = (base_ref[...].astype(jnp.float32) + value).astype(jnp.bfloat16)


def product(info, own, other, w, base, name):
    rows, width = own.shape
    features = w.shape[0]
    tall = features // 4
    return pl.pallas_call(
        product_kernel,
        grid_spec=pltpu.PrefetchScalarGridSpec(
            num_scalar_prefetch=1,
            grid=(4,),
            in_specs=[
                pl.BlockSpec((rows, width), lambda i, s: (0, 0)),
                pl.BlockSpec((rows, width), lambda i, s: (0, 0)),
                pl.BlockSpec((tall, 2 * width), lambda i, s: (i, 0)),
                pl.BlockSpec((rows, tall), lambda i, s: (0, i)),
            ],
            out_specs=pl.BlockSpec((rows, tall), lambda i, s: (0, i)),
            scratch_shapes=[pltpu.VMEM((rows, 2 * width), jnp.bfloat16)],
        ),
        out_shape=jax.ShapeDtypeStruct((rows, features), jnp.bfloat16),
        compiler_params=pltpu.CompilerParams(
            dimension_semantics=("arbitrary",), vmem_limit_bytes=40 * 2**20
        ),
        cost_estimate=pl.CostEstimate(
            flops=2 * rows * features * 2 * width, bytes_accessed=4 * features * width, transcendentals=0
        ),
        name=name,
    )(info, own, other, w, base)


def pick(left, right):
    return jnp.dot(left, right, preferred_element_type=jnp.float32).astype(jnp.bfloat16)


def body(
    grad_top,
    in_weight,
    out_weight,
    gate_branch,
    write_vec,
    read_vec,
    log_decay,
    step_size,
    skip_gain,
    visual_pos,
    visual_count,
    visual_owner,
    visual_patch,
):
    x_at, z_at, core = lax.axis_index(X), lax.axis_index(Z), lax.axis_index(C)
    seq_count = lax.axis_size(SEQ)
    seq_index = lax.axis_index(SEQ)
    sign = 1 - 2 * core
    grad_rows = grad_top[0]
    tok_rows, model_width = grad_rows.shape
    n = write_vec.shape[2]
    heads = log_decay.shape[1] // 2
    info = jnp.stack([core, x_at, z_at]).astype(jnp.int32)

    rows_y = lax.all_gather(jnp.concatenate([out_weight, in_weight], axis=1), Y, axis=0, tiled=True)
    w_out_rows, w_in_rows = rows_y[:, : out_weight.shape[1]], rows_y[:, out_weight.shape[1] :]
    w_in_full = lax.all_gather(w_in_rows, SEQ, axis=0, tiled=True)

    w_mine = half_of(w_out_rows, core, 1)
    w_other = swap_cores(half_of(w_out_rows, 1 - core, 1))
    w_chip = chip_rows(w_mine, w_other, core)
    part = w_chip.shape[1] // 2
    pieces = []
    places = []
    for color, (first, second) in enumerate(((X, Z), (Z, X))):
        own = w_chip[:, color * part : (color + 1) * part]
        plane = jnp.stack([own] + [send(own, first, s) for s in (1, 2, 3)])
        for k2 in range(4):
            pieces.append(plane)
            if k2 < 3:
                plane = send(plane, second, 1)
            for k1 in range(4):
                kx, kz = (k1, k2) if color == 0 else (k2, k1)
                places.append(lax.rem(x_at - sign * kx + 4, 4) * 4 + lax.rem(z_at - sign * kz + 4, 4))
    place = jnp.stack(places).astype(jnp.int32)

    x_other = swap_cores(grad_rows)
    gate_other = swap_cores(half_of(gate_branch[0], 1 - core, 1))
    vectors = jnp.stack([write_vec[0], read_vec[0]])
    write, read = chip_rows(vectors, swap_cores(vectors), core, axis=1)
    scalars_other = swap_cores(
        jnp.concatenate([half_of(log_decay[0], 1 - core, 0), half_of(step_size[0], 1 - core, 0)])
    )
    skip = jnp.repeat(half_of(skip_gain, core, 0), 64)[None]
    heads_map = jnp.asarray(np.tile(np.repeat(np.eye(heads), 64, axis=1), (2, 1)), jnp.bfloat16)
    u, v, row, extra = decays(info, log_decay[0], step_size[0], scalars_other, heads_map)

    owner_row = visual_owner[0]
    patch_row = visual_patch[0]
    count_row = visual_count[0]
    slot_count = owner_row.shape[1]
    slot_ids = jnp.arange(slot_count)
    live_slot = slot_ids[None, :] < count_row[:, None]
    earlier_slot = slot_ids[None, :] < slot_ids[:, None]
    same_owner = (
        (owner_row[:, :, None] == owner_row[:, None, :])
        & live_slot[:, None, :]
        & earlier_slot[None]
    )
    rank_row = jnp.sum(same_owner.astype(jnp.int32), axis=2)
    own_owner = lax.dynamic_index_in_dim(owner_row, seq_index, 0, keepdims=False)
    own_rank = lax.dynamic_index_in_dim(rank_row, seq_index, 0, keepdims=False)
    own_live = lax.dynamic_index_in_dim(live_slot, seq_index, 0, keepdims=False)
    destination = own_owner * CAP + own_rank
    send_columns = jnp.arange(seq_count * CAP)
    send_map = ((send_columns[:, None] == destination[None, :]) & own_live[None, :]).astype(jnp.bfloat16)
    pos_map = (visual_pos[0, 0][:, None] == jnp.arange(tok_rows)[None, :]).astype(jnp.bfloat16)
    take = jnp.dot(send_map, pos_map, preferred_element_type=jnp.float32).astype(jnp.bfloat16)

    def arrived(sent):
        sent = sent.reshape(seq_count, CAP, sent.shape[1])
        return lax.all_to_all(sent, SEQ, 0, 0, tiled=True).reshape(seq_count * CAP, sent.shape[2])

    def exchange(rows):
        return arrived(pick(take, rows))

    mine_mask = live_slot & (owner_row == seq_index)
    column = jnp.arange(seq_count)[:, None] * CAP + rank_row
    patch_count = seq_count * CAP
    patch_hit = (
        (patch_row.reshape(-1)[:, None] == jnp.arange(patch_count)[None, :])
        & mine_mask.reshape(-1)[:, None]
    ).astype(jnp.bfloat16)
    column_hit = (column.reshape(-1)[:, None] == send_columns[None, :]).astype(jnp.bfloat16)
    select = lax.dot_general(
        patch_hit, column_hit, (((0,), (0,)), ((), ())), preferred_element_type=jnp.float32
    ).astype(jnp.bfloat16)
    placed = lambda rows: jnp.dot(select, rows, preferred_element_type=jnp.float32)

    grad_patches = placed(exchange(grad_rows)).astype(jnp.bfloat16)
    place, grad_patches, take, select = lax.optimization_barrier((place, grad_patches, take, select))

    gated, gated_v, local, share = gated_and_states(
        info, place, pieces, grad_rows, x_other, gate_branch[0], gate_other, read, v, row, extra, heads_map
    )

    share = lax.all_to_all(share, (X, Z), 0, 0, tiled=True)
    inflow = lax.all_to_all(suffix(share, heads_map), (X, Z), 0, 0, tiled=True).reshape(n, -1)
    inner = functools.partial(
        inner_gradient, info, write, read, u, gated, gated_v, local, inflow, row, skip, heads_map
    )
    inner_other = swap_cores(inner(False))
    inner_own = inner(True)

    first = core == 0
    mine, theirs = pick(take, inner_own), pick(take, inner_other)
    rows = jnp.concatenate([jnp.where(first, mine, theirs), jnp.where(first, theirs, mine)], axis=1)
    patch_rows = placed(arrived(rows)).astype(jnp.bfloat16)
    half = patch_rows.shape[1] // 2
    result = product(info, inner_own, inner_other, w_in_full, grad_rows, "product_tokens")
    low, high = patch_rows[:, :half], patch_rows[:, half:]
    patches = product(
        info, jnp.where(first, low, high), jnp.where(first, high, low), w_in_full, grad_patches, "product_patches"
    )
    return (result[None], patches[None])


def solution(mesh):
    finer = Mesh(mesh.devices.reshape(SIZES), ALL)
    return jax.shard_map(
        body,
        mesh=finer,
        in_specs=(
            P(Y, SEQ, None),
            P(ALL, None),
            P(ALL, None),
            P(Y, SEQ, None),
            P(Y, SEQ, None),
            P(Y, SEQ, None),
            P(Y, None, SEQ),
            P(Y, None, SEQ),
            P(),
            P(Y, SEQ, None),
            P(Y, None),
            P(Y, None, None),
            P(Y, None, None),
        ),
        out_specs=(P(Y, SEQ, None), P(Y, SEQ, None)),
        check_vma=False,
    )
```
